32 devices in a mesh: row: 8 (over z, x), col: 4 (over y, core).
Axes of the slice: x: 2, y: 2, z: 4, core: 2. Of those that a mesh axis runs over, the one named last changes fastest.
Arguments:
- pole_values: float32 [65536], P('row'), may hold values from -32768 to 32768, as said below
- weights: float32 [65536], P('row'), may hold values from 0.15 to 0.5
- centers: float32 [65536], P('col'), as said below
- offsets: float32 [65536], P('col'), may hold values from -0.1 to 0.1
- chosen: int32 [2048], replicated, may hold values from 0 to 65535
- column_pole: int32 [2, 32768], P(None, 'row'), may hold values from 0 to 65535, as said below
- eigen_blocks: bfloat16 [3072, 2, 32768], P('col', None, 'row'), may hold values from -6 to 6
Outputs:
- roots_offset: float32 [65536], P('col')
- panel: float32 [3072, 2, 2048], P(('col', 'row'))
The draws below stay inside these ranges and needn't reach their ends.
Inputs may be any that keep to these rules, and one draw needn't show every extreme that they name: `pole_values`: ascending; consecutive poles differ by 1/4 to 7/4; every pole is a multiple of 1/128. centers[i] is the midpoint of pole_values[i] and pole_values[i + 1]; the last one is the last pole plus 1/2. `chosen`: indices of roots. `column_pole`: each of 0 to 65535 stands once.
All inputs are finite; a program needn't handle non-finite values.
Results may differ from the reference program's by a relative error of at most 0.0021.
Values may be sent and summed in bfloat16 or wider, within the bound.
A program may use at most 128 MiB of HBM per device.

```python
import math
import jax
import jax.numpy as jnp
from jax import lax

N = 65536
H = 32768
ITERS = 3
K = 2048
QROWS = 3072


def pole_layout(key):
    marks = jax.random.randint(jax.random.fold_in(key, 11), (N,), 16, 113)
    return (jnp.arange(N) - N // 2).astype(jnp.float32) + marks.astype(jnp.float32) / 128.0


def draw_pole_values(key, part):
    return pole_layout(key)


def draw_centers(key, part):
    values = pole_layout(key)
    return jnp.concatenate([0.5 * (values[:-1] + values[1:]), values[-1:] + 0.5])


def draw_column_pole(key, part):
    return jax.random.permutation(jax.random.fold_in(key, 5), N).astype(jnp.int32).reshape(2, H)


def plant(drawn, stream_key, smallest, high):
    shape = drawn.shape
    place = [jax.random.randint(jax.random.fold_in(stream_key, axis), (), 0, shape[axis]) for axis in range(len(shape))]
    drawn = drawn.at[tuple(place)].set(smallest)
    longest = shape.index(max(shape))
    place[longest] = (place[longest] + 1) % shape[longest]
    return drawn.at[tuple(place)].set(high)


def steps_of(own_key, shape, shards, smallest, top_value):
    factor_of = 1.0
    for dim, shards_of in shards:
        heights = jax.random.uniform(jax.random.fold_in(jax.random.fold_in(own_key, 6), dim), (shards_of,), jnp.float32, smallest / len(shards), top_value / len(shards))
        factor_of = factor_of * jnp.repeat(jnp.exp(heights), shape[dim] // shards_of).reshape((-1,) + (1,) * (len(shape) - 1 - dim))
    return factor_of


def gaussian(key, dims, scale, most, split=(), dtype=jnp.bfloat16):
    entries = jax.random.normal(key, dims, jnp.float32) * scale
    if len(split) > 0:
        entries = steps_of(key, dims, split, -0.22, 0.18) * entries
    return jnp.clip(entries, min=-most, max=most).astype(dtype)


def setup_inputs(seed: int = 0) -> dict:
    key_of = jax.random.split(jax.random.key(seed), 8)
    pole_values = draw_pole_values(jax.random.fold_in(key_of[7], 71), 0)
    weights = jnp.clip(jnp.exp(math.log(0.5) - 1.2039728 * jax.random.uniform(key_of[1], (N,), jnp.float32) ** steps_of(key_of[1], (N,), ((0, 8),), -0.2, 0.2)), 0.15, 0.5)
    centers = draw_centers(jax.random.fold_in(key_of[7], 71), 0)
    offsets = jnp.clip(jax.random.uniform(key_of[3], (N,), jnp.float32, -0.1, 0.1) * steps_of(key_of[3], (N,), ((0, 4),), -0.4, 0.0), -0.1, 0.1)
    chosen = plant(jax.random.randint(key_of[4], (K,), 0, N), jax.random.fold_in(key_of[4], 1), 0, N - 1).astype(jnp.int32)
    column_pole = draw_column_pole(jax.random.fold_in(key_of[7], 71), 0)
    eigen_blocks = gaussian(key_of[6], (QROWS, 2, H), 1.0, 6.0, ((0, 4), (2, 8)))
    return {"pole_values": pole_values, "weights": weights, "centers": centers, "offsets": offsets, "chosen": chosen, "column_pole": column_pole, "eigen_blocks": eigen_blocks}


def block_sums(pole_vals, weight_sq, center_vals, offset_vals, block_rows):
    root_count = center_vals.shape[0]
    block_rows = min(block_rows, root_count)
    center_blocks = center_vals.reshape(root_count // block_rows, block_rows)
    offset_blocks = offset_vals.reshape(root_count // block_rows, block_rows)

    def per_block(blocks):
        distance = pole_vals[None, :] - blocks[0][:, None] - blocks[1][:, None]
        inverse = 1.0 / distance
        weighted = weight_sq[None, :] * inverse
        return (lax.optimization_barrier(jnp.sum(weighted, axis=1)), lax.optimization_barrier(jnp.sum(weighted * inverse, axis=1)), lax.optimization_barrier(jnp.min(jnp.abs(distance), axis=1)))
    sums = lax.map(per_block, (center_blocks, offset_blocks))
    return tuple((item.reshape(root_count) for item in sums))

def newton_update(offset_now, sum_inverse, sum_square, nearest):
    limit = 0.5 * nearest
    return offset_now - jnp.clip((1.0 + sum_inverse) / sum_square, -limit, limit)

def cauchy_block(pole_picked, weight_picked, panel_center, panel_offset, inv_norm):
    distance = pole_picked[:, None] - panel_center[None, :] - panel_offset[None, :]
    return (weight_picked[:, None] * (1.0 / distance) * inv_norm[None, :]).astype(jnp.bfloat16)

def reference(pole_values, weights, centers, offsets, chosen, column_pole, eigen_blocks):
    weight_sq = weights * weights
    offset_now = offsets
    for iteration in range(ITERS):
        sum_inverse, sum_square, nearest = block_sums(pole_values, weight_sq, centers, offset_now, 128)
        offset_now = newton_update(offset_now, sum_inverse, sum_square, nearest)
    panel_center = centers[chosen]
    panel_offset = offset_now[chosen]
    norm_sq = block_sums(pole_values, weight_sq, panel_center, panel_offset, 64)[1]
    inv_norm = lax.rsqrt(norm_sq)
    halves_out = []
    for half_index in range(2):
        pole_index = column_pole[half_index]
        cauchy = cauchy_block(pole_values[pole_index], weights[pole_index], panel_center, panel_offset, inv_norm)
        halves_out.append(jnp.dot(eigen_blocks[:, half_index, :], cauchy, preferred_element_type=jnp.float32))
    return (offset_now, jnp.stack(halves_out, axis=1))
```

```python
import itertools
import jax
import jax.numpy as jnp
from jax import lax
from jax.experimental import pallas as pl
from jax.experimental.pallas import tpu as pltpu
from jax.sharding import PartitionSpec as P

AXES = ("row", "col")
LANES=128
ITERS=3
BLOCK=32
TERMS=40
KAPPA=12.0
SPLIT=4

def power(base, exponent):
    result = jnp.ones_like(base)
    square = base
    for bit in range(6):
        result = jnp.where((exponent >> bit) & 1 == 1, result * square, result)
        square = square * square
    return result

def pieces(values):
    high = values.astype(jnp.bfloat16).astype(jnp.float32)
    return high, values - high

def coefficients(geometry_ref, block_poles_ref, block_weights_ref, coeff_ref, top_ref, bottom_ref):
    chunks = block_poles_ref.shape[0]
    tiles = coeff_ref.shape[0]
    blank = jnp.zeros((8, LANES), jnp.float32)
    for k in range(BLOCK, TERMS):
        top_ref[8 * k : 8 * k + 8, :] = blank
        bottom_ref[8 * k : 8 * k + 8, :] = blank

    for octet in range(geometry_ref.shape[1] // 8):
        middle, radius, first, last = (geometry_ref[i, 8 * octet : 8 * octet + 8, :] for i in range(4))
        inverse_radius = 1.0 / radius

        def chunk(q, _):
            block = (q * LANES + lax.broadcasted_iota(jnp.int32, (8, LANES), 1)).astype(jnp.float32)
            far = jnp.logical_or(block < first, block >= last)
            scale = jnp.where(far, radius, 0.0)
            top, bottom = [], [jnp.ones((8, LANES), jnp.float32)]
            for j in range(BLOCK):
                ratio = scale / (block_poles_ref[q, j : j + 1, :] - middle)
                value = block_weights_ref[q, j : j + 1, :] * ratio * inverse_radius
                new_top, new_bottom = [], []
                for k in range(j + 1):
                    term = value * bottom[k]
                    if k < j:
                        term = top[k] + term
                    if k > 0:
                        term = term - ratio * top[k - 1]
                    new_top.append(term)
                for k in range(j + 2):
                    term = bottom[k] if k <= j else None
                    if k > 0:
                        shifted = ratio * bottom[k - 1]
                        term = -shifted if term is None else term - shifted
                    new_bottom.append(term)
                top, bottom = new_top, new_bottom
            for k in range(BLOCK):
                top_ref[8 * k : 8 * k + 8, :] = top[k]
            for k in range(BLOCK + 1):
                bottom_ref[8 * k : 8 * k + 8, :] = bottom[k]
            for member in range(8):
                tile = 8 * octet + member
                if tile >= tiles:
                    continue
                for ref, at in ((top_ref, 0), (bottom_ref, LANES)):
                    high, low = pieces(ref[pl.ds(member, TERMS, stride=8), :])
                    rows = jnp.concatenate([high, low, high, blank], axis=0)
                    coeff_ref[tile, q, :, at : at + LANES] = rows.astype(jnp.bfloat16)
            return 0

        lax.fori_loop(0, chunks, chunk, 0)


def roots_kernel(near_ref, middle_ref, radius_ref, geometry_ref, block_poles_ref, block_weights_ref, poles_ref, weight_sq_ref,
                 center_ref, offset_ref, left_ref, right_ref, out_ref, coeff_ref, top_ref, bottom_ref):
    coefficients(geometry_ref, block_poles_ref, block_weights_ref, coeff_ref, top_ref, bottom_ref)
    tiles, chunks = coeff_ref.shape[0], coeff_ref.shape[1]
    order = lax.broadcasted_iota(jnp.int32, (TERMS, LANES), 0)
    blank = jnp.zeros((8, LANES), jnp.float32)
    out_ref[...] = offset_ref[...]

    def to_rows(values):
        high, low = pieces(values)
        return jnp.concatenate([high, high, low, blank], axis=0).T.astype(jnp.bfloat16)

    def update(index, _):
        tile = lax.rem(index, tiles)
        center = center_ref[pl.ds(tile, 1), :]
        offset = out_ref[pl.ds(tile, 1), :]
        middle, radius = middle_ref[tile], radius_ref[tile]
        place = (center - middle) + offset
        ratio = jnp.broadcast_to(place / radius, (TERMS, LANES))
        value_rows = to_rows(power(ratio, order))
        slope_rows = to_rows(order.astype(jnp.float32) * power(ratio, jnp.maximum(order - 1, 0)))
        rows = jnp.concatenate([value_rows, slope_rows], axis=0)

        def far(step, sums):
            inverse_sum, square_sum = sums
            for i in range(SPLIT):
                got = jnp.dot(rows, coeff_ref[tile, step * SPLIT + i], preferred_element_type=jnp.float32)
                top, bottom = got[:LANES, :LANES], got[:LANES, LANES:]
                top_slope, bottom_slope = got[LANES:, :LANES], got[LANES:, LANES:]
                inverse = 1.0 / bottom
                quotient = top * inverse
                inverse_sum = inverse_sum + quotient
                square_sum = square_sum + (top_slope - quotient * bottom_slope) * inverse
            return inverse_sum, square_sum

        zero = jnp.zeros((LANES, LANES), jnp.float32)
        inverse_sum, square_sum = lax.fori_loop(0, chunks // SPLIT, far, (zero, zero))
        place_rows = jnp.broadcast_to(place, (LANES, LANES)).T

        def near(row, sums):
            inverse_sum, square_sum = sums
            pole = poles_ref[pl.ds(row, 1), :] - middle
            inverse = 1.0 / (pole - place_rows)
            weighted = weight_sq_ref[pl.ds(row, 1), :] * inverse
            return inverse_sum + weighted, square_sum + weighted * inverse

        inverse_sum, square_sum = lax.fori_loop(near_ref[0, tile], near_ref[1, tile], near, (inverse_sum, square_sum / radius))
        sum_inverse = jnp.sum(inverse_sum.T, axis=0, keepdims=True)
        sum_square = jnp.sum(square_sum.T, axis=0, keepdims=True)
        to_left = left_ref[pl.ds(tile, 1), :] - center
        to_right = right_ref[pl.ds(tile, 1), :] - center
        limit = 0.5 * jnp.minimum(jnp.abs(to_left - offset), jnp.abs(to_right - offset))
        change = (1.0 + sum_inverse) / sum_square
        out_ref[pl.ds(tile, 1), :] = offset - jnp.minimum(jnp.maximum(change, -limit), limit)
        return 0

    lax.fori_loop(0, ITERS * tiles, update, 0)


def find_roots(poles, weight_sq, centers, offsets, left, right):
    flat = lambda values: values.reshape(-1, LANES)
    tiles = centers.shape[0] // LANES
    chunks = poles.shape[0] // (BLOCK * LANES)
    tile_centers = flat(centers)
    middle = tile_centers[:, LANES // 2]
    radius = jnp.maximum(tile_centers[:, -1] - middle, middle - tile_centers[:, 0]) + 2.5
    below = jnp.sum((poles[None, :] <= (middle - KAPPA * radius)[:, None]).astype(jnp.int32), axis=1)
    inside = jnp.sum((poles[None, :] < (middle + KAPPA * radius)[:, None]).astype(jnp.int32), axis=1)
    near = jnp.stack([below // LANES, (inside + LANES - 1) // LANES])
    per_row = LANES // BLOCK
    geometry = jnp.stack([middle, radius, (near[0] * per_row).astype(jnp.float32), (near[1] * per_row).astype(jnp.float32)])
    geometry = jnp.pad(geometry, ((0, 0), (0, -tiles % 8)), mode="edge")
    geometry = jnp.broadcast_to(geometry[:, :, None], geometry.shape + (LANES,))
    blocked = lambda values: values.reshape(chunks, LANES, BLOCK).transpose(0, 2, 1)
    smem, vmem = pl.BlockSpec(memory_space=pltpu.SMEM), pl.BlockSpec(memory_space=pltpu.VMEM)
    return pl.pallas_call(
        roots_kernel,
        out_shape=jax.ShapeDtypeStruct((tiles, LANES), jnp.float32),
        in_specs=[smem] * 3 + [vmem] * 9,
        out_specs=vmem,
        scratch_shapes=[
            pltpu.VMEM((tiles, chunks, LANES, 2 * LANES), jnp.bfloat16),
            pltpu.VMEM((8 * TERMS, LANES), jnp.float32),
            pltpu.VMEM((8 * TERMS, LANES), jnp.float32),
        ],
        compiler_params=pltpu.CompilerParams(vmem_limit_bytes=48 * 1024 * 1024),
        cost_estimate=pl.CostEstimate(flops=200_000_000_000, bytes_accessed=2_000_000, transcendentals=0),
        name="roots",
    )(near, middle, radius, geometry, blocked(poles), blocked(weight_sq), flat(poles), flat(weight_sq), tile_centers, flat(offsets), flat(left), flat(right)).reshape(-1)


def gather(items, collective_id):
    sizes = {axis: lax.axis_size(axis) for axis in AXES}
    offsets_of = lambda axes: list(itertools.product(*[range(sizes[a]) if a in axes else (0,) for a in AXES]))
    groups = [offsets_of(axes) for _, axes in items]
    greeted = max(groups, key=len)[1:]
    count = len(items)

    def kernel(*refs):
        sources, targets, send, receive = refs[:count], refs[count : 2 * count], refs[2 * count], refs[2 * count + 1]
        here = [lax.axis_index(axis) for axis in AXES]
        device = lambda offset: tuple(lax.rem(h + o, sizes[a]) for h, o, a in zip(here, offset, AXES))
        barrier = pltpu.get_barrier_semaphore()
        for offset in greeted:
            pl.semaphore_signal(barrier, inc=1, device_id=device(offset), device_id_type=pl.DeviceIdType.MESH)
        pl.semaphore_wait(barrier, len(greeted))
        copies = []
        for (_, axes), group, source, target in zip(items, groups, sources, targets):
            slot = 0
            for h, a in zip(here, AXES):
                if a in axes:
                    slot = slot * sizes[a] + h
            for offset in group[1:]:
                copies.append(
                    pltpu.make_async_remote_copy(
                        src_ref=source,
                        dst_ref=target.at[slot],
                        send_sem=send.at[len(copies)],
                        recv_sem=receive.at[len(copies)],
                        device_id=device(offset),
                        device_id_type=pl.DeviceIdType.MESH,
                    )
                )
                copies[-1].start()
            target[slot] = source[...]
        for copy in copies:
            copy.wait()

    total = sum(len(group) - 1 for group in groups)
    vmem = pl.BlockSpec(memory_space=pltpu.VMEM)
    return pl.pallas_call(
        kernel,
        out_shape=[jax.ShapeDtypeStruct((len(g),) + v.shape, v.dtype) for (v, _), g in zip(items, groups)],
        in_specs=[vmem] * count,
        out_specs=[vmem] * count,
        scratch_shapes=[pltpu.SemaphoreType.DMA((total,)), pltpu.SemaphoreType.DMA((total,))],
        compiler_params=pltpu.CompilerParams(collective_id=collective_id, has_side_effects=True),
        name="gather",
    )(*[v for v, _ in items])


def chosen_kernel(poles_ref, weight_sq_ref, center_ref, offset_ref, left_ref, right_ref, offset_out_ref, norm_ref):
    center = center_ref[...]
    to_left = left_ref[...] - center
    to_right = right_ref[...] - center
    rows = poles_ref.shape[0]

    def sweep(offset, square_only):
        def row(index, sums):
            inverse = 1.0 / ((poles_ref[pl.ds(index, 1), :] - center) - offset)
            weighted = weight_sq_ref[pl.ds(index, 1), :] * inverse
            square_sum = sums[1] + weighted * inverse
            return (sums[0] if square_only else sums[0] + weighted), square_sum

        zero = jnp.zeros_like(center)
        sums = lax.fori_loop(0, rows, row, (zero, zero), unroll=4)
        return [jnp.broadcast_to(jnp.sum(s, axis=1, keepdims=True), center.shape) for s in sums]

    def step(_, offset):
        sum_inverse, sum_square = sweep(offset, False)
        limit = 0.5 * jnp.minimum(jnp.abs(to_left - offset), jnp.abs(to_right - offset))
        change = (1.0 + sum_inverse) / sum_square
        return offset - jnp.minimum(jnp.maximum(change, -limit), limit)

    offset = lax.fori_loop(0, ITERS, step, offset_ref[...])
    offset_out_ref[...] = offset
    norm_ref[...] = lax.rsqrt(sweep(offset, True)[1])


def find_chosen(poles, weight_sq, center, offset, left, right):
    flat = lambda values: values.reshape(-1, LANES)
    wide = lambda values: jnp.broadcast_to(values[:, None], values.shape + (LANES,))
    vmem = pl.BlockSpec(memory_space=pltpu.VMEM)
    found = jax.ShapeDtypeStruct(center.shape + (LANES,), jnp.float32)
    offset, norm = pl.pallas_call(
        chosen_kernel, out_shape=[found, found], in_specs=[vmem] * 6, out_specs=[vmem] * 2, name="chosen"
    )(flat(poles), flat(weight_sq), wide(center), wide(offset), wide(left), wide(right))
    return offset[:, 0], norm[:, 0]


def lookup(tables, index):
    rows = jnp.concatenate([t.reshape(-1, LANES) for t in tables], axis=1)
    high = lax.reduce_precision(rows, 8, 7)
    middle = lax.reduce_precision(rows - high, 8, 7)
    low = (rows - high) - middle
    pieces = jnp.concatenate([high, middle, low], axis=1).astype(jnp.bfloat16)
    pick = (index[:, None] // LANES == jnp.arange(rows.shape[0])[None, :]).astype(jnp.bfloat16)
    found = jnp.dot(pick, pieces, preferred_element_type=jnp.float32)
    width = rows.shape[1]
    found = (found[:, :width] + found[:, width : 2 * width]) + found[:, 2 * width :]
    lane = index[:, None] % LANES == jnp.arange(LANES)[None, :]
    return [
        jnp.sum(jnp.where(lane, found[:, t * LANES : (t + 1) * LANES], 0.0), axis=1)
        for t in range(len(tables))
    ]


def on_device(pole_values, weights, centers, offsets, chosen, column_pole, eigen_blocks):
    flat = lambda values: values.reshape(-1, LANES)
    rows, cols = lax.axis_size("row"), lax.axis_size("col")
    row, col = lax.axis_index("row"), lax.axis_index("col")
    per_device = offsets.shape[0] // rows
    first_root = row * per_device
    my_first = col * offsets.shape[0] + first_root
    my_centers = lax.dynamic_slice_in_dim(centers, first_root, per_device)
    my_offsets = lax.dynamic_slice_in_dim(offsets, first_root, per_device)
    all_poles, all_weights, all_offsets = gather(
        [(flat(pole_values), ("row",)), (flat(weights), ("row",)), (flat(my_offsets), AXES)], 0
    )
    all_poles, all_weights = all_poles.reshape(-1), all_weights.reshape(-1)
    all_offsets = all_offsets.reshape(rows, cols, per_device).transpose(1, 0, 2).reshape(-1)
    weight_sq = all_weights * all_weights
    shifted = jnp.concatenate([all_poles[1:], all_poles[-1:]])

    share = chosen.shape[0] // (rows * cols)
    mine = lax.dynamic_slice_in_dim(chosen, (row * cols + col) * share, share)
    left, right, start = lookup([all_poles, shifted, all_offsets], mine)
    center = jnp.where(mine == all_poles.shape[0] - 1, left + 0.5, 0.5 * (left + right))
    offset, inverse_norm = find_chosen(all_poles, weight_sq, center, start, left, right)
    packed = jnp.pad(jnp.stack([center, offset, inverse_norm]), ((0, 5), (0, LANES - share)))
    panel = gather([(packed, AXES)], 1)[0][:, :3, :share].transpose(1, 0, 2).reshape(3, -1)
    panel_center, panel_offset, inv_norm = panel[0], panel[1], panel[2]

    pole_picked, weight_picked = lookup([all_poles, all_weights], column_pole.reshape(-1))
    pole_picked = pole_picked.reshape(column_pole.shape)
    weight_picked = weight_picked.reshape(column_pole.shape)
    received = []
    for half in range(column_pole.shape[0]):
        distance = (pole_picked[half][:, None] - panel_center[None, :]) - panel_offset[None, :]
        cauchy = (weight_picked[half][:, None] * (1.0 / distance) * inv_norm[None, :]).astype(jnp.bfloat16)
        part = jnp.dot(eigen_blocks[:, half, :], cauchy, preferred_element_type=jnp.float32)
        sent = part.astype(jnp.bfloat16).reshape(rows, -1, part.shape[1])
        received.append(lax.all_to_all(sent, "row", split_axis=0, concat_axis=0, tiled=True))

    my_left = lax.dynamic_slice_in_dim(all_poles, my_first, per_device)
    my_right = lax.dynamic_slice_in_dim(shifted, my_first, per_device)
    my_offsets = find_roots(all_poles, weight_sq, my_centers, my_offsets, my_left, my_right)
    offset_now = gather([(flat(my_offsets), ("row",))], 2)[0].reshape(-1)
    halves = [jnp.sum(got.astype(jnp.float32), axis=0) for got in received]
    return (offset_now, jnp.stack(halves, axis=1))


def solution(mesh):
    placed = (P("row"), P("row"), P("col"), P("col"), P(), P(None, "row"), P("col", None, "row"))
    return jax.shard_map(
        on_device,
        mesh=mesh,
        in_specs=placed,
        out_specs=(P("col"), P(("col", "row"), None, None)),
        check_vma=False,
    )
```

```python
import itertools
import jax
import jax.numpy as jnp
from jax import lax
from jax.experimental import pallas as pl
from jax.experimental.pallas import tpu as pltpu
from jax.sharding import PartitionSpec as P

AXES = ("row", "col")
LANES = 128
ITERS = 3
BLOCK = 32
TERMS = 40
KAPPA = 8.0
PAIR = 2
PIECES = 3
WIDTH = 256
DEPTH = 1024
PARTS = 2
FLOPS_PER_US = 1_000_000_000


def power(base, exponent):
    result = jnp.ones_like(base)
    square = base
    for bit in range(6):
        result = jnp.where((exponent >> bit) & 1 == 1, result * square, result)
        square = square * square
    return result


def pieces(values):
    high = values.astype(jnp.bfloat16).astype(jnp.float32)
    return high, values - high


def gather(items, collective_id):
    sizes = {axis: lax.axis_size(axis) for axis in AXES}
    offsets_of = lambda axes: list(itertools.product(*[range(sizes[a]) if a in axes else (0,) for a in AXES]))
    groups = [offsets_of(axes) for _, axes in items]
    greeted = sorted({offset for group in groups for offset in group[1:]})
    count = len(items)

    def kernel(*refs):
        sources, targets, send, receive = refs[:count], refs[count : 2 * count], refs[2 * count], refs[2 * count + 1]
        here = [lax.axis_index(axis) for axis in AXES]
        device = lambda offset: tuple(lax.rem(h + o, sizes[a]) for h, o, a in zip(here, offset, AXES))
        barrier = pltpu.get_barrier_semaphore()
        for offset in greeted:
            pl.semaphore_signal(barrier, inc=1, device_id=device(offset), device_id_type=pl.DeviceIdType.MESH)
        pl.semaphore_wait(barrier, len(greeted))
        copies = []
        for (_, axes), group, source, target in zip(items, groups, sources, targets):
            slot = 0
            for h, a in zip(here, AXES):
                if a in axes:
                    slot = slot * sizes[a] + h
            for offset in group[1:]:
                copies.append(
                    pltpu.make_async_remote_copy(
                        src_ref=source,
                        dst_ref=target.at[slot],
                        send_sem=send.at[len(copies)],
                        recv_sem=receive.at[len(copies)],
                        device_id=device(offset),
                        device_id_type=pl.DeviceIdType.MESH,
                    )
                )
                copies[-1].start()
            target[slot] = source[...]
        for copy in copies:
            copy.wait()

    total = sum(len(group) - 1 for group in groups)
    vmem = pl.BlockSpec(memory_space=pltpu.VMEM)
    return pl.pallas_call(
        kernel,
        out_shape=[jax.ShapeDtypeStruct((len(g),) + v.shape, v.dtype) for (v, _), g in zip(items, groups)],
        in_specs=[vmem] * count,
        out_specs=[vmem] * count,
        scratch_shapes=[pltpu.SemaphoreType.DMA((total,)), pltpu.SemaphoreType.DMA((total,))],
        compiler_params=pltpu.CompilerParams(collective_id=collective_id, has_side_effects=True),
        name="gather",
    )(*[v for v, _ in items])


def coefficients_kernel(geometry_ref, block_poles_ref, block_weights_ref, *refs):
    coeff_ref, top_ref, bottom_ref = refs[-3:]
    q = pl.program_id(1)
    blank = jnp.zeros((8, LANES), jnp.float32)
    for k in range(BLOCK, TERMS):
        top_ref[8 * k : 8 * k + 8, :] = blank
        bottom_ref[8 * k : 8 * k + 8, :] = blank
    middle, radius, first, last = (geometry_ref[i] for i in range(4))
    inverse_radius = 1.0 / radius
    block = (q * LANES + lax.broadcasted_iota(jnp.int32, (8, LANES), 1)).astype(jnp.float32)
    far = jnp.logical_or(block < first, block >= last)
    scale = jnp.where(far, radius, 0.0)
    top, bottom = [], [jnp.ones((8, LANES), jnp.float32)]
    for j in range(BLOCK):
        weight = block_weights_ref[0, j : j + 1, :]
        ratio = scale / (block_poles_ref[0, j : j + 1, :] - middle)
        value = (weight * weight) * ratio * inverse_radius
        new_top, new_bottom = [], []
        for k in range(j + 1):
            term = value * bottom[k]
            if k < j:
                term = top[k] + term
            if k > 0:
                term = term - ratio * top[k - 1]
            new_top.append(term)
        for k in range(j + 2):
            term = bottom[k] if k <= j else None
            if k > 0:
                shifted = ratio * bottom[k - 1]
                term = -shifted if term is None else term - shifted
            new_bottom.append(term)
        top, bottom = new_top, new_bottom
    for k in range(BLOCK):
        top_ref[8 * k : 8 * k + 8, :] = top[k]
    for k in range(BLOCK + 1):
        bottom_ref[8 * k : 8 * k + 8, :] = bottom[k]
    for member in range(coeff_ref.shape[0]):
        for ref, at in ((top_ref, 0), (bottom_ref, LANES)):
            high, low = pieces(ref[pl.ds(member, TERMS, stride=8), :])
            rows = jnp.concatenate([high, low, high, blank], axis=0)
            coeff_ref[member, 0, :, at : at + LANES] = rows.astype(jnp.bfloat16)


def update_kernel(near_ref, middle_ref, radius_ref, first_ref, poles_ref, weights_ref, center_ref, offset_ref, coeff_ref, *refs):
    out_ref = refs[-1]
    tile = pl.program_id(0)
    chunks = coeff_ref.shape[1]
    order = lax.broadcasted_iota(jnp.int32, (TERMS, LANES), 0)
    blank = jnp.zeros((8, LANES), jnp.float32)

    def to_rows(values):
        high, low = pieces(values)
        return jnp.concatenate([high, high, low, blank], axis=0).T.astype(jnp.bfloat16)

    center, offset = center_ref[0], offset_ref[0]
    middle, radius = middle_ref[tile], radius_ref[tile]
    place = (center - middle) + offset
    ratio = jnp.broadcast_to(place / radius, (TERMS, LANES))
    value_rows = to_rows(power(ratio, order))
    slope_rows = to_rows(order.astype(jnp.float32) * power(ratio, jnp.maximum(order - 1, 0)))
    rows = jnp.concatenate([value_rows, slope_rows], axis=0)
    inverse_sum = square_sum = None
    for q in range(chunks):
        got = jnp.dot(rows, coeff_ref[0, q], preferred_element_type=jnp.float32)
        top, bottom = got[:LANES, :LANES], got[:LANES, LANES:]
        top_slope, bottom_slope = got[LANES:, :LANES], got[LANES:, LANES:]
        inverse = 1.0 / bottom
        quotient = top * inverse
        slope = (top_slope - quotient * bottom_slope) * inverse
        inverse_sum = quotient if q == 0 else inverse_sum + quotient
        square_sum = slope if q == 0 else square_sum + slope
    square_sum = square_sum / radius
    place_rows = jnp.broadcast_to(place, (LANES, LANES)).T
    inverse_parts, square_parts = [], []
    half = LANES // 2
    for part in range(2):
        own = slice(part * half, (part + 1) * half)
        points = place_rows[own]

        def near(step, sums):
            inverse_sum, square_sum = sums
            for i in range(PAIR):
                row = step * PAIR + i
                pole = poles_ref[pl.ds(row, 1), :] - middle
                weight = weights_ref[pl.ds(row, 1), :]
                inverse = 1.0 / (pole - points)
                weighted = (weight * weight) * inverse
                inverse_sum = inverse_sum + weighted
                square_sum = square_sum + weighted * inverse
            return inverse_sum, square_sum

        sums = lax.fori_loop(near_ref[0, tile], near_ref[1, tile], near, (inverse_sum[own], square_sum[own]))
        inverse_parts.append(sums[0])
        square_parts.append(sums[1])
    total = lambda parts: jnp.sum(jnp.concatenate(parts, axis=0).T, axis=0, keepdims=True)
    sum_inverse, sum_square = total(inverse_parts), total(square_parts)
    row = first_ref[0] + tile
    to_left = poles_ref[pl.ds(row, 1), :] - center
    final = lax.broadcasted_iota(jnp.int32, (1, LANES), 1) + row * LANES == poles_ref.shape[0] * LANES - 1
    to_right = jnp.where(final, to_left, -to_left)
    limit = 0.5 * jnp.minimum(jnp.abs(to_left - offset), jnp.abs(to_right - offset))
    change = (1.0 + sum_inverse) / sum_square
    out_ref[0] = offset - jnp.minimum(jnp.maximum(change, -limit), limit)


def find_roots(poles, weights, centers, offsets, my_first, after):
    flat = lambda values: values.reshape(-1, LANES)
    tiles = centers.shape[0] // LANES
    chunks = poles.shape[0] // (BLOCK * LANES)
    tile_centers = flat(centers)
    middle = tile_centers[:, LANES // 2]
    radius = jnp.maximum(tile_centers[:, -1] - middle, middle - tile_centers[:, 0]) + 2.5
    below = jnp.sum((poles[None, :] <= (middle - KAPPA * radius)[:, None]).astype(jnp.int32), axis=1)
    inside = jnp.sum((poles[None, :] < (middle + KAPPA * radius)[:, None]).astype(jnp.int32), axis=1)
    unit = PAIR * LANES
    near = jnp.stack([below // unit, (inside + unit - 1) // unit])
    limits = (near * (unit // BLOCK)).astype(jnp.float32)
    octet = min(tiles, 8)
    geometry = jnp.stack([middle, radius, limits[0], limits[1]])
    geometry = jnp.pad(geometry, ((0, 0), (0, -tiles % 8)), mode="edge")
    geometry = jnp.broadcast_to(geometry[:, :, None], geometry.shape + (LANES,))
    blocked = lambda values: values.reshape(chunks, LANES, BLOCK).transpose(0, 2, 1)
    smem, anywhere = pl.BlockSpec(memory_space=pltpu.SMEM), pl.BlockSpec(memory_space=pl.ANY)
    coeff = pl.pallas_call(
        coefficients_kernel,
        grid=(geometry.shape[1] // 8, chunks),
        out_shape=jax.ShapeDtypeStruct((tiles, chunks, LANES, 2 * LANES), jnp.bfloat16),
        in_specs=[
            pl.BlockSpec((4, 8, LANES), lambda o, q: (0, o, 0)),
            pl.BlockSpec((1, BLOCK, LANES), lambda o, q: (q, 0, 0)),
            pl.BlockSpec((1, BLOCK, LANES), lambda o, q: (q, 0, 0)),
        ] + [anywhere] * len(after[0]),
        out_specs=pl.BlockSpec((octet, 1, LANES, 2 * LANES), lambda o, q: (o, q, 0, 0)),
        scratch_shapes=[pltpu.VMEM((8 * TERMS, LANES), jnp.float32)] * 2,
        cost_estimate=pl.CostEstimate(flops=FLOPS_PER_US * 18, bytes_accessed=tiles * chunks * LANES * LANES * 4, transcendentals=0),
        name="coefficients",
    )(geometry, blocked(poles), blocked(weights), *after[0])
    whole = pl.BlockSpec((poles.shape[0] // LANES, LANES), lambda t: (0, 0))
    one = pl.BlockSpec((1, 1, LANES), lambda t: (t, 0, 0))
    spread = lambda values: values.reshape(tiles, 1, LANES)
    now = spread(offsets)
    first = (my_first // LANES).reshape(1)
    for step in range(ITERS):
        now = pl.pallas_call(
            update_kernel,
            grid=(tiles,),
            out_shape=jax.ShapeDtypeStruct((tiles, 1, LANES), jnp.float32),
            in_specs=[smem] * 4 + [whole] * 2 + [one] * 2 + [pl.BlockSpec((1, chunks, LANES, 2 * LANES), lambda t: (t, 0, 0, 0))] + [anywhere] * len(after[step + 1]),
            out_specs=one,
            cost_estimate=pl.CostEstimate(flops=FLOPS_PER_US * 18, bytes_accessed=tiles * chunks * LANES * LANES * 4, transcendentals=0),
            name="update",
        )(near, middle, radius, first, flat(poles), flat(weights), spread(centers), now, coeff, *after[step + 1])
    return now.reshape(-1)


def lookup_kernel(index_ref, *refs):
    count = (len(refs) - 1) // 2
    tables, targets, pieces_ref = refs[:count], refs[count : 2 * count], refs[2 * count]
    rows = tables[0].shape[0]

    @pl.when(pl.program_id(0) == 0)
    def _():
        for t, table in enumerate(tables):
            rest = table[...]
            for p in range(PIECES):
                part = rest.astype(jnp.bfloat16)
                at = (t * PIECES + p) * LANES
                pieces_ref[:, at : at + LANES] = part
                rest = rest - part.astype(jnp.float32)

    lane = lax.broadcasted_iota(jnp.int32, (LANES, LANES), 1)
    for g in range(index_ref.shape[0]):
        index = jnp.broadcast_to(index_ref[g], (LANES, LANES)).T
        high = lax.shift_right_logical(index, 7)
        low = lax.bitwise_and(index, LANES - 1)
        pick = jnp.concatenate([(high == lane + c * LANES).astype(jnp.float32) for c in range(rows // LANES)], axis=1)
        found = jnp.dot(pick.astype(jnp.bfloat16), pieces_ref[...], preferred_element_type=jnp.float32)
        for t, target in enumerate(targets):
            parts = [found[:, (t * PIECES + p) * LANES : (t * PIECES + p + 1) * LANES] for p in range(PIECES)]
            value = (parts[0] + parts[1]) + parts[2]
            value = jnp.sum(jnp.where(low == lane, value, 0.0), axis=1, keepdims=True)
            target[g * LANES : (g + 1) * LANES, :] = jnp.broadcast_to(value, (LANES, LANES))


def lookup(tables, index):
    groups = index.shape[0] // LANES
    step = min(groups, 8)
    count = len(tables)
    return pl.pallas_call(
        lookup_kernel,
        grid=(groups // step,),
        out_shape=[jax.ShapeDtypeStruct((index.shape[0], LANES), jnp.float32)] * count,
        in_specs=[pl.BlockSpec((step, 1, LANES), lambda i: (i, 0, 0))] + [pl.BlockSpec(t.shape, lambda i: (0, 0)) for t in tables],
        out_specs=[pl.BlockSpec((step * LANES, LANES), lambda i: (i, 0))] * count,
        scratch_shapes=[pltpu.VMEM((tables[0].shape[0], count * PIECES * LANES), jnp.bfloat16)],
        name="lookup",
    )(index.reshape(groups, 1, LANES), *tables)


def chosen_kernel(poles_ref, weights_ref, last_ref, left_ref, right_ref, start_ref, out_ref):
    count = last_ref.shape[0]
    left, right = left_ref[:count], right_ref[:count]
    center = jnp.where(last_ref[...] > 0, left + 0.5, 0.5 * (left + right))
    to_left, to_right = left - center, right - center
    rows = poles_ref.shape[0]

    def sweep(offset, square_only):
        def row(index, sums):
            inverse = 1.0 / ((poles_ref[pl.ds(index, 1), :] - center) - offset)
            weight = weights_ref[pl.ds(index, 1), :]
            weighted = (weight * weight) * inverse
            square_sum = sums[1] + weighted * inverse
            return (sums[0] if square_only else sums[0] + weighted), square_sum

        zero = jnp.zeros_like(center)
        sums = lax.fori_loop(0, rows, row, (zero, zero), unroll=8)
        return [jnp.broadcast_to(jnp.sum(s, axis=1, keepdims=True), center.shape) for s in sums]

    def step(_, offset):
        sum_inverse, sum_square = sweep(offset, False)
        limit = 0.5 * jnp.minimum(jnp.abs(to_left - offset), jnp.abs(to_right - offset))
        change = (1.0 + sum_inverse) / sum_square
        return offset - jnp.minimum(jnp.maximum(change, -limit), limit)

    offset = lax.fori_loop(0, ITERS, step, start_ref[:count])
    norm = lax.rsqrt(sweep(offset, True)[1])
    lane = lax.broadcasted_iota(jnp.int32, (count, LANES), 1)
    own = lane == lax.broadcasted_iota(jnp.int32, (count, LANES), 0)
    spread = lambda values: jnp.sum(jnp.where(own, values, 0.0), axis=0, keepdims=True)
    blank = jnp.zeros((5, LANES), jnp.float32)
    out_ref[...] = jnp.concatenate([spread(center), spread(offset), spread(norm), blank], axis=0)


def panel_kernel(side_ref, pole_ref, weight_ref, center_ref, offset_ref, norm_ref, eigen_ref, send_ref, keep_ref, total_ref):
    depth = eigen_ref.shape[2]
    center, offset, norm = center_ref[...], offset_ref[...], norm_ref[...]
    total = None
    for first in range(0, depth, DEPTH):
        rows = slice(first, first + DEPTH)
        columns = []
        for at in range(0, WIDTH, LANES):
            lanes = slice(at, at + LANES)
            distance = (pole_ref[rows, :] - center[:, lanes]) - offset[:, lanes]
            columns.append((weight_ref[rows, :] * (1.0 / distance) * norm[:, lanes]).astype(jnp.bfloat16))
        part = jnp.dot(eigen_ref[0, :, rows], jnp.concatenate(columns, axis=1), preferred_element_type=jnp.float32)
        total = part if total is None else total + part
    total_ref[...] = total
    side = side_ref[0]
    size = send_ref.shape[1]
    for z in range(send_ref.shape[0]):
        send_ref[z] = total_ref[pl.ds(pl.multiple_of((2 * z + 1 - side) * size, 8), size), :].astype(jnp.bfloat16)
        keep_ref[z] = total_ref[pl.ds(pl.multiple_of((2 * z + side) * size, 8), size), :]


def panel_part(side, pole, weight, panel, eigen, half, first, width, rows):
    height, depth = eigen.shape[1], eigen.shape[2]
    shape = (rows // 2, height // rows, width)
    row = pl.BlockSpec((1, WIDTH), lambda i: (0, first // WIDTH + i))
    wide = pl.BlockSpec((depth, LANES), lambda i: (half, 0))
    out = pl.BlockSpec(shape[:2] + (WIDTH,), lambda i: (0, 0, i))
    return pl.pallas_call(
        panel_kernel,
        grid=(width // WIDTH,),
        out_shape=[jax.ShapeDtypeStruct(shape, jnp.bfloat16), jax.ShapeDtypeStruct(shape, jnp.float32)],
        in_specs=[pl.BlockSpec(memory_space=pltpu.SMEM), wide, wide, row, row, row, pl.BlockSpec((1, height, depth), lambda i: (half, 0, 0))],
        out_specs=[out, out],
        scratch_shapes=[pltpu.VMEM((height, WIDTH), jnp.float32)],
        cost_estimate=pl.CostEstimate(flops=FLOPS_PER_US * 9, bytes_accessed=height * depth * 2, transcendentals=0),
        compiler_params=pltpu.CompilerParams(vmem_limit_bytes=56 * 1024 * 1024),
        name="panel",
    )(side, pole, weight, *[p[None, :] for p in panel], eigen)


def on_device(pole_values, weights, centers, offsets, chosen, column_pole, eigen_blocks):
    flat = lambda values: values.reshape(-1, LANES)
    rows, cols = lax.axis_size("row"), lax.axis_size("col")
    row, col = lax.axis_index("row"), lax.axis_index("col")
    per_device = offsets.shape[0] // rows
    first_root = row * per_device
    my_first = col * offsets.shape[0] + first_root
    all_poles, all_weights, all_offsets = gather_inputs(pole_values, weights, offsets)
    total = all_poles.shape[0]

    share = chosen.shape[0] // (rows * cols)
    mine = lax.dynamic_slice_in_dim(chosen, (row * cols + col) * share, share)
    padded = jnp.pad(mine, (0, LANES - share))
    index = jnp.concatenate([padded, jnp.minimum(padded + 1, total - 1)])
    found_pole, found_offset = lookup([flat(all_poles), flat(all_offsets)], index)
    last = jnp.broadcast_to((mine == total - 1).astype(jnp.int32)[:, None], (share, LANES))
    here = pl.BlockSpec(memory_space=pltpu.VMEM)
    packed = pl.pallas_call(
        chosen_kernel, out_shape=jax.ShapeDtypeStruct((8, LANES), jnp.float32), in_specs=[here] * 6, out_specs=here, name="chosen"
    )(flat(all_poles), flat(all_weights), last, found_pole[:LANES], found_pole[LANES:], found_offset[:LANES])
    panel = gather([(packed, AXES)], 1)[0][:, :3, :share].transpose(1, 0, 2).reshape(3, -1)

    pole, weight = lookup([flat(all_poles), flat(all_weights)], column_pole.reshape(-1))
    eigen = jnp.transpose(eigen_blocks, (1, 0, 2))
    side = lax.rem(row, 2).reshape(1)
    deep = row // 2
    near_pairs = [(r, r ^ 1) for r in range(rows)]
    received, outgoing = [], []
    width = chosen.shape[0] // PARTS
    for half in range(column_pole.shape[0]):
        for first in range(0, chosen.shape[0], width):
            send, keep = panel_part(side, pole, weight, panel, eigen, half, first, width, rows)
            met = lax.ppermute(send, "row", near_pairs)
            both = keep + met.astype(jnp.float32)
            blocks, arrived = [], [lax.dynamic_index_in_dim(both, deep, 0, keepdims=False)]
            for shift in range(1, rows // 2):
                block = lax.dynamic_index_in_dim(both, lax.rem(deep + shift, rows // 2), 0, keepdims=False)
                blocks.append(block.astype(jnp.bfloat16))
                pairs = [(r, (r + 2 * shift) % rows) for r in range(rows)]
                arrived.append(lax.ppermute(blocks[-1], "row", pairs))
            outgoing.append(blocks)
            received.append(arrived)

    my_centers = lax.dynamic_slice_in_dim(centers, first_root, per_device)
    my_offsets = lax.dynamic_slice_in_dim(offsets, first_root, per_device)
    after = [outgoing[0] + outgoing[1], outgoing[2], outgoing[3], []]
    my_offsets = find_roots(all_poles, all_weights, my_centers, my_offsets, my_first, after)
    offset_now = gather([(flat(my_offsets), ("row",))], 2)[0].reshape(-1)
    add = lambda parts: sum([p.astype(jnp.float32) for p in parts[1:]], parts[0])
    halves = [jnp.concatenate([add(parts) for parts in received[at : at + PARTS]], axis=1) for at in range(0, len(received), PARTS)]
    return (offset_now, jnp.stack(halves, axis=1))


def gather_inputs(pole_values, weights, offsets):
    flat = lambda values: values.reshape(-1, LANES)
    all_poles, all_weights, all_offsets = gather([(flat(pole_values), ("row",)), (flat(weights), ("row",)), (flat(offsets), ("col",))], 0)
    return all_poles.reshape(-1), all_weights.reshape(-1), all_offsets.reshape(-1)


def solution(mesh):
    placed = (P("row"), P("row"), P("col"), P("col"), P(), P(None, "row"), P("col", None, "row"))

    return jax.shard_map(
        on_device,
        mesh=mesh,
        in_specs=placed,
        out_specs=(P("col"), P(("col", "row"), None, None)),
        check_vma=False,
    )
```

```python
import functools
import itertools
import jax
import jax.numpy as jnp
from jax import lax
from jax.experimental import pallas as pl
from jax.experimental.pallas import tpu as pltpu
from jax.sharding import PartitionSpec as P

AXES = ("row", "col")
LANES = 128
ITERS = 3
BLOCK = 32
TERMS = 40
KAPPA = 8.0
PAIR = 2
PIECES = 3
WIDTH = 256
DEPTH = 1024
FLOPS_PER_US = 1_000_000_000


def power(base, exponent):
    result = jnp.ones_like(base)
    square = base
    for bit in range(6):
        result = jnp.where((exponent >> bit) & 1 == 1, result * square, result)
        square = square * square
    return result


def pieces(values):
    high = values.astype(jnp.bfloat16).astype(jnp.float32)
    return high, values - high


def gather(items, collective_id):
    sizes = {axis: lax.axis_size(axis) for axis in AXES}
    offsets_of = lambda axes: list(itertools.product(*[range(sizes[a]) if a in axes else (0,) for a in AXES]))
    groups = [offsets_of(axes) for _, axes in items]
    greeted = sorted({offset for group in groups for offset in group[1:]})
    count = len(items)

    def kernel(*refs):
        sources, targets, send, receive = refs[:count], refs[count : 2 * count], refs[2 * count], refs[2 * count + 1]
        here = [lax.axis_index(axis) for axis in AXES]
        device = lambda offset: tuple(lax.rem(h + o, sizes[a]) for h, o, a in zip(here, offset, AXES))
        barrier = pltpu.get_barrier_semaphore()
        for offset in greeted:
            pl.semaphore_signal(barrier, inc=1, device_id=device(offset), device_id_type=pl.DeviceIdType.MESH)
        pl.semaphore_wait(barrier, len(greeted))
        copies = []
        for (_, axes), group, source, target in zip(items, groups, sources, targets):
            slot = 0
            for h, a in zip(here, AXES):
                if a in axes:
                    slot = slot * sizes[a] + h
            for offset in group[1:]:
                copies.append(
                    pltpu.make_async_remote_copy(
                        src_ref=source,
                        dst_ref=target.at[slot],
                        send_sem=send.at[len(copies)],
                        recv_sem=receive.at[len(copies)],
                        device_id=device(offset),
                        device_id_type=pl.DeviceIdType.MESH,
                    )
                )
                copies[-1].start()
            target[slot] = source[...]
        for copy in copies:
            copy.wait()

    total = sum(len(group) - 1 for group in groups)
    vmem = pl.BlockSpec(memory_space=pltpu.VMEM)
    return pl.pallas_call(
        kernel,
        out_shape=[jax.ShapeDtypeStruct((len(g),) + v.shape, v.dtype) for (v, _), g in zip(items, groups)],
        in_specs=[vmem] * count,
        out_specs=[vmem] * count,
        scratch_shapes=[pltpu.SemaphoreType.DMA((total,)), pltpu.SemaphoreType.DMA((total,))],
        compiler_params=pltpu.CompilerParams(collective_id=collective_id, has_side_effects=True),
        name="gather",
    )(*[v for v, _ in items])


def coefficients(geometry, poles, weights, q, coeff_ref, at, top_ref, bottom_ref):
    blank = jnp.zeros((8, LANES), jnp.float32)
    for k in range(BLOCK, TERMS):
        top_ref[8 * k : 8 * k + 8, :] = blank
        bottom_ref[8 * k : 8 * k + 8, :] = blank
    middle, radius, first, last = geometry
    inverse_radius = 1.0 / radius
    block = (q * LANES + lax.broadcasted_iota(jnp.int32, (8, LANES), 1)).astype(jnp.float32)
    far = jnp.logical_or(block < first, block >= last)
    scale = jnp.where(far, radius, 0.0)
    top, bottom = [], [jnp.ones((8, LANES), jnp.float32)]
    for j in range(BLOCK):
        weight = weights[j : j + 1, :]
        ratio = scale / (poles[j : j + 1, :] - middle)
        value = (weight * weight) * ratio * inverse_radius
        new_top, new_bottom = [], []
        for k in range(j + 1):
            term = value * bottom[k]
            if k < j:
                term = top[k] + term
            if k > 0:
                term = term - ratio * top[k - 1]
            new_top.append(term)
        for k in range(j + 2):
            term = bottom[k] if k <= j else None
            if k > 0:
                shifted = ratio * bottom[k - 1]
                term = -shifted if term is None else term - shifted
            new_bottom.append(term)
        top, bottom = new_top, new_bottom
    for k in range(BLOCK):
        top_ref[8 * k : 8 * k + 8, :] = top[k]
    for k in range(BLOCK + 1):
        bottom_ref[8 * k : 8 * k + 8, :] = bottom[k]
    for member in range(coeff_ref.shape[0]):
        for ref, lane in ((top_ref, 0), (bottom_ref, LANES)):
            high, low = pieces(ref[pl.ds(member, TERMS, stride=8), :])
            rows = jnp.concatenate([high, low, high, blank], axis=0)
            coeff_ref[member, at, :, lane : lane + LANES] = rows.astype(jnp.bfloat16)


def update_kernel(count, base, near_ref, middle_ref, radius_ref, first_ref, poles_ref, weights_ref, center_ref, offset_ref, *refs):
    coeff_refs, out_ref = refs[:count], refs[-1]
    step = pl.program_id(0)
    tile = base + step
    order = lax.broadcasted_iota(jnp.int32, (TERMS, LANES), 0)
    blank = jnp.zeros((8, LANES), jnp.float32)

    def to_rows(values):
        high, low = pieces(values)
        return jnp.concatenate([high, high, low, blank], axis=0).T.astype(jnp.bfloat16)

    center, offset = center_ref[0], offset_ref[0]
    middle, radius = middle_ref[tile], radius_ref[tile]
    place = (center - middle) + offset
    ratio = jnp.broadcast_to(place / radius, (TERMS, LANES))
    value_rows = to_rows(power(ratio, order))
    slope_rows = to_rows(order.astype(jnp.float32) * power(ratio, jnp.maximum(order - 1, 0)))
    rows = jnp.concatenate([value_rows, slope_rows], axis=0)
    inverse_sum = square_sum = None
    for ref, q in [(ref, q) for ref in coeff_refs for q in range(ref.shape[1])]:
        got = jnp.dot(rows, ref[0, q], preferred_element_type=jnp.float32)
        top, bottom = got[:LANES, :LANES], got[:LANES, LANES:]
        top_slope, bottom_slope = got[LANES:, :LANES], got[LANES:, LANES:]
        inverse = 1.0 / bottom
        quotient = top * inverse
        slope = (top_slope - quotient * bottom_slope) * inverse
        inverse_sum = quotient if inverse_sum is None else inverse_sum + quotient
        square_sum = slope if square_sum is None else square_sum + slope
    square_sum = square_sum / radius
    place_rows = jnp.broadcast_to(place, (LANES, LANES)).T
    inverse_parts, square_parts = [], []
    half = LANES // 2
    for part in range(2):
        own = slice(part * half, (part + 1) * half)
        points = place_rows[own]

        def near(step, sums):
            inverse_sum, square_sum = sums
            for i in range(PAIR):
                row = step * PAIR + i
                pole = poles_ref[pl.ds(row, 1), :] - middle
                weight = weights_ref[pl.ds(row, 1), :]
                inverse = 1.0 / (pole - points)
                weighted = (weight * weight) * inverse
                inverse_sum = inverse_sum + weighted
                square_sum = square_sum + weighted * inverse
            return inverse_sum, square_sum

        sums = lax.fori_loop(near_ref[0, tile], near_ref[1, tile], near, (inverse_sum[own], square_sum[own]))
        inverse_parts.append(sums[0])
        square_parts.append(sums[1])
    total = lambda parts: jnp.sum(jnp.concatenate(parts, axis=0).T, axis=0, keepdims=True)
    sum_inverse, sum_square = total(inverse_parts), total(square_parts)
    row = first_ref[0] + tile
    to_left = poles_ref[pl.ds(row, 1), :] - center
    final = lax.broadcasted_iota(jnp.int32, (1, LANES), 1) + row * LANES == poles_ref.shape[0] * LANES - 1
    to_right = jnp.where(final, to_left, -to_left)
    limit = 0.5 * jnp.minimum(jnp.abs(to_left - offset), jnp.abs(to_right - offset))
    change = (1.0 + sum_inverse) / sum_square
    out_ref[0] = offset - jnp.minimum(jnp.maximum(change, -limit), limit)


def prepare(poles, weights, centers):
    flat = lambda values: values.reshape(-1, LANES)
    tiles = centers.shape[0] // LANES
    chunks = poles.shape[0] // (BLOCK * LANES)
    tile_centers = flat(centers)
    middle = tile_centers[:, LANES // 2]
    radius = jnp.maximum(tile_centers[:, -1] - middle, middle - tile_centers[:, 0]) + 2.5
    below = jnp.sum((poles[None, :] <= (middle - KAPPA * radius)[:, None]).astype(jnp.int32), axis=1)
    inside = jnp.sum((poles[None, :] < (middle + KAPPA * radius)[:, None]).astype(jnp.int32), axis=1)
    unit = PAIR * LANES
    near = jnp.stack([below // unit, (inside + unit - 1) // unit])
    limits = (near * (unit // BLOCK)).astype(jnp.float32)
    geometry = jnp.stack([middle, radius, limits[0], limits[1]])
    geometry = jnp.pad(geometry, ((0, 0), (0, -tiles % 8)), mode="edge")
    geometry = jnp.broadcast_to(geometry[:, :, None], geometry.shape + (LANES,))
    blocked = lambda values: values.reshape(chunks, LANES, BLOCK).transpose(0, 2, 1)
    return near, middle, radius, geometry, blocked(poles), blocked(weights)


def update(prepared, poles, weights, centers, now, my_first, base, coeffs, after):
    near, middle, radius = prepared[:3]
    flat = lambda values: values.reshape(-1, LANES)
    smem, anywhere = pl.BlockSpec(memory_space=pltpu.SMEM), pl.BlockSpec(memory_space=pl.ANY)
    whole = pl.BlockSpec((poles.shape[0] // LANES, LANES), lambda t: (0, 0))
    tiles = coeffs[0].shape[0]
    one = pl.BlockSpec((1, 1, LANES), lambda t: (t, 0, 0))
    return pl.pallas_call(
        functools.partial(update_kernel, len(coeffs), base),
        grid=(tiles,),
        out_shape=jax.ShapeDtypeStruct((tiles, 1, LANES), jnp.float32),
        in_specs=[smem] * 4
        + [whole] * 2
        + [pl.BlockSpec((1, 1, LANES), lambda t: (base + t, 0, 0)), one]
        + [pl.BlockSpec((1,) + c.shape[1:], lambda t: (t, 0, 0, 0)) for c in coeffs]
        + [anywhere] * len(after),
        out_specs=one,
        cost_estimate=pl.CostEstimate(flops=FLOPS_PER_US * 10, bytes_accessed=tiles * LANES * LANES * 64, transcendentals=0),
        name="update",
    )(near, middle, radius, (my_first // LANES).reshape(1), flat(poles), flat(weights), centers.reshape(-1, 1, LANES), now, *coeffs, *after)


def lookup_kernel(index_ref, *refs):
    count = (len(refs) - 1) // 2
    tables, targets, pieces_ref = refs[:count], refs[count : 2 * count], refs[2 * count]
    rows = tables[0].shape[0]

    @pl.when(pl.program_id(0) == 0)
    def _():
        for t, table in enumerate(tables):
            rest = table[...]
            for p in range(PIECES):
                part = rest.astype(jnp.bfloat16)
                at = (t * PIECES + p) * LANES
                pieces_ref[:, at : at + LANES] = part
                rest = rest - part.astype(jnp.float32)

    lane = lax.broadcasted_iota(jnp.int32, (LANES, LANES), 1)
    for g in range(index_ref.shape[0]):
        index = jnp.broadcast_to(index_ref[g], (LANES, LANES)).T
        high = lax.shift_right_logical(index, 7)
        low = lax.bitwise_and(index, LANES - 1)
        pick = jnp.concatenate([(high == lane + c * LANES).astype(jnp.float32) for c in range(rows // LANES)], axis=1)
        found = jnp.dot(pick.astype(jnp.bfloat16), pieces_ref[...], preferred_element_type=jnp.float32)
        for t, target in enumerate(targets):
            parts = [found[:, (t * PIECES + p) * LANES : (t * PIECES + p + 1) * LANES] for p in range(PIECES)]
            value = (parts[0] + parts[1]) + parts[2]
            value = jnp.sum(jnp.where(low == lane, value, 0.0), axis=1, keepdims=True)
            target[g * LANES : (g + 1) * LANES, :] = jnp.broadcast_to(value, (LANES, LANES))


def lookup(tables, index):
    groups = index.shape[0] // LANES
    step = min(groups, 8)
    count = len(tables)
    return pl.pallas_call(
        lookup_kernel,
        grid=(groups // step,),
        out_shape=[jax.ShapeDtypeStruct((index.shape[0], LANES), jnp.float32)] * count,
        in_specs=[pl.BlockSpec((step, 1, LANES), lambda i: (i, 0, 0))] + [pl.BlockSpec(t.shape, lambda i: (0, 0)) for t in tables],
        out_specs=[pl.BlockSpec((step * LANES, LANES), lambda i: (i, 0))] * count,
        scratch_shapes=[pltpu.VMEM((tables[0].shape[0], count * PIECES * LANES), jnp.bfloat16)],
        name="lookup",
    )(index.reshape(groups, 1, LANES), *tables)


def chosen_kernel(poles_ref, weights_ref, last_ref, left_ref, right_ref, start_ref, out_ref):
    count = last_ref.shape[0]
    left, right = left_ref[:count], right_ref[:count]
    center = jnp.where(last_ref[...] > 0, left + 0.5, 0.5 * (left + right))
    to_left, to_right = left - center, right - center
    rows = poles_ref.shape[0]

    def sweep(offset, square_only):
        def row(index, sums):
            inverse = 1.0 / ((poles_ref[pl.ds(index, 1), :] - center) - offset)
            weight = weights_ref[pl.ds(index, 1), :]
            weighted = (weight * weight) * inverse
            square_sum = sums[1] + weighted * inverse
            return (sums[0] if square_only else sums[0] + weighted), square_sum

        zero = jnp.zeros_like(center)
        sums = lax.fori_loop(0, rows, row, (zero, zero), unroll=8)
        return [jnp.broadcast_to(jnp.sum(s, axis=1, keepdims=True), center.shape) for s in sums]

    def step(_, offset):
        sum_inverse, sum_square = sweep(offset, False)
        limit = 0.5 * jnp.minimum(jnp.abs(to_left - offset), jnp.abs(to_right - offset))
        change = (1.0 + sum_inverse) / sum_square
        return offset - jnp.minimum(jnp.maximum(change, -limit), limit)

    offset = lax.fori_loop(0, ITERS, step, start_ref[:count])
    norm = lax.rsqrt(sweep(offset, True)[1])
    lane = lax.broadcasted_iota(jnp.int32, (count, LANES), 1)
    own = lane == lax.broadcasted_iota(jnp.int32, (count, LANES), 0)
    spread = lambda values: jnp.sum(jnp.where(own, values, 0.0), axis=0, keepdims=True)
    blank = jnp.zeros((5, LANES), jnp.float32)
    out_ref[...] = jnp.concatenate([spread(center), spread(offset), spread(norm), blank], axis=0)


def panel_kernel(start, chunks, side_ref, pole_ref, weight_ref, center_ref, offset_ref, norm_ref, eigen_ref, geometry_ref, block_poles_ref, block_weights_ref, send_ref, keep_ref, coeff_ref, total_ref, *refs):
    depth = eigen_ref.shape[2]
    center, offset, norm = center_ref[...], offset_ref[...], norm_ref[...]
    total = None
    for first in range(0, depth, DEPTH):
        rows = slice(first, first + DEPTH)
        columns = []
        for at in range(0, WIDTH, LANES):
            lanes = slice(at, at + LANES)
            distance = (pole_ref[rows, :] - center[:, lanes]) - offset[:, lanes]
            columns.append((weight_ref[rows, :] * (1.0 / distance) * norm[:, lanes]).astype(jnp.bfloat16))
        part = jnp.dot(eigen_ref[0, :, rows], jnp.concatenate(columns, axis=1), preferred_element_type=jnp.float32)
        total = part if total is None else total + part
    per = coeff_ref.shape[1]
    for u in range(per):
        q = lax.rem(start + pl.program_id(0) * per + u, chunks)
        geometry = [geometry_ref[i] for i in range(4)]
        coefficients(geometry, block_poles_ref[u], block_weights_ref[u], q, coeff_ref, u, *refs[2 * u : 2 * u + 2])
    total_ref[...] = total
    side = side_ref[0]
    size = send_ref.shape[1]
    for z in range(send_ref.shape[0]):
        send_ref[z] = total_ref[pl.ds(pl.multiple_of((2 * z + 1 - side) * size, 8), size), :].astype(jnp.bfloat16)
        keep_ref[z] = total_ref[pl.ds(pl.multiple_of((2 * z + side) * size, 8), size), :]


def panel_half(side, pole, weight, panel, eigen, half, rows, prepared, tiles):
    height, depth = eigen.shape[1], eigen.shape[2]
    width = panel[0].shape[0]
    steps = width // WIDTH
    geometry, block_poles, block_weights = prepared[3:]
    chunks = block_poles.shape[0]
    octets = geometry.shape[1] // 8
    per = octets * chunks // (eigen.shape[0] * steps)
    start = half * steps * per
    octet, members = start // chunks, min(tiles, 8)
    shape = (rows // 2, height // rows, width)
    row = pl.BlockSpec((1, WIDTH), lambda i: (0, i))
    wide = pl.BlockSpec((depth, LANES), lambda i: (half, 0))
    out = pl.BlockSpec(shape[:2] + (WIDTH,), lambda i: (0, 0, i))
    blocks = pl.BlockSpec((per, BLOCK, LANES), lambda i: (start % chunks // per + i, 0, 0))
    return pl.pallas_call(
        functools.partial(panel_kernel, start, chunks),
        grid=(steps,),
        out_shape=[
            jax.ShapeDtypeStruct(shape, jnp.bfloat16),
            jax.ShapeDtypeStruct(shape, jnp.float32),
            jax.ShapeDtypeStruct((members, steps * per, LANES, 2 * LANES), jnp.bfloat16),
        ],
        in_specs=[pl.BlockSpec(memory_space=pltpu.SMEM), wide, wide, row, row, row, pl.BlockSpec((1, height, depth), lambda i: (half, 0, 0))]
        + [pl.BlockSpec((4, 8, LANES), lambda i: (0, octet, 0)), blocks, blocks],
        out_specs=[out, out, pl.BlockSpec((members, per, LANES, 2 * LANES), lambda i: (0, i, 0, 0))],
        scratch_shapes=[pltpu.VMEM((height, WIDTH), jnp.float32)] + [pltpu.VMEM((8 * TERMS, LANES), jnp.float32)] * (2 * per),
        cost_estimate=pl.CostEstimate(flops=FLOPS_PER_US * 22, bytes_accessed=height * depth * 2, transcendentals=0),
        compiler_params=pltpu.CompilerParams(vmem_limit_bytes=60 * 1024 * 1024),
        name="panel",
    )(side, pole, weight, *[p[None, :] for p in panel], eigen, geometry, block_poles, block_weights)


def merge_kernel(deep_ref, keep_ref, met_ref, own_ref, *block_refs):
    count = keep_ref.shape[0]
    deep = deep_ref[0]
    for shift, ref in enumerate((own_ref,) + block_refs):
        at = lax.rem(deep + shift, count)
        ref[...] = (keep_ref[at] + met_ref[at].astype(jnp.float32)).astype(ref.dtype)


def merge(deep, keep, met):
    count, height, width = keep.shape
    size = WIDTH * 2
    whole = pl.BlockSpec((count, height, size), lambda i: (0, 0, i))
    block = pl.BlockSpec((height, size), lambda i: (0, i))
    return pl.pallas_call(
        merge_kernel,
        grid=(width // size,),
        out_shape=[jax.ShapeDtypeStruct((height, width), jnp.bfloat16 if s else jnp.float32) for s in range(count)],
        in_specs=[pl.BlockSpec(memory_space=pltpu.SMEM), whole, whole],
        out_specs=[block] * count,
        cost_estimate=pl.CostEstimate(flops=FLOPS_PER_US * 2, bytes_accessed=keep.size * 8, transcendentals=0),
        name="merge",
    )(deep.reshape(1), keep, met)


def on_device(pole_values, weights, centers, offsets, chosen, column_pole, eigen_blocks):
    flat = lambda values: values.reshape(-1, LANES)
    rows, cols = lax.axis_size("row"), lax.axis_size("col")
    row, col = lax.axis_index("row"), lax.axis_index("col")
    per_device = offsets.shape[0] // rows
    first_root = row * per_device
    my_first = col * offsets.shape[0] + first_root
    all_poles, all_weights, all_offsets = gather_inputs(pole_values, weights, offsets, rows, cols)
    total = all_poles.shape[0]

    share = chosen.shape[0] // (rows * cols)
    mine = lax.dynamic_slice_in_dim(chosen, (row * cols + col) * share, share)
    padded = jnp.pad(mine, (0, LANES - share))
    per_col = offsets.shape[0]
    turned = lax.rem(col - padded // per_col + cols, cols) * per_col + lax.rem(padded, per_col)
    index = jnp.concatenate([padded, jnp.minimum(padded + 1, total - 1), turned])
    found_pole, found_offset = lookup([flat(all_poles), all_offsets], index)
    last = jnp.broadcast_to((mine == total - 1).astype(jnp.int32)[:, None], (share, LANES))
    here = pl.BlockSpec(memory_space=pltpu.VMEM)
    packed = pl.pallas_call(
        chosen_kernel, out_shape=jax.ShapeDtypeStruct((8, LANES), jnp.float32), in_specs=[here] * 6, out_specs=here, name="chosen"
    )(flat(all_poles), flat(all_weights), last, found_pole[:LANES], found_pole[LANES : 2 * LANES], found_offset[2 * LANES :])
    shared = copies(packed, AXES, rows * cols)
    panel = shared[:, :3, :share].transpose(1, 0, 2).reshape(3, -1)

    pole, weight = lookup([flat(all_poles), flat(all_weights)], column_pole.reshape(-1))
    eigen = jnp.transpose(eigen_blocks, (1, 0, 2))
    side = lax.rem(row, 2).reshape(1)
    deep = row // 2
    near_pairs = [(r, r ^ 1) for r in range(rows)]
    my_centers = lax.dynamic_slice_in_dim(centers, first_root, per_device)
    my_offsets = lax.dynamic_slice_in_dim(offsets, first_root, per_device)
    prepared = prepare(all_poles, all_weights, my_centers)
    tiles = per_device // LANES
    received, outgoing, coeffs = [], [], []
    for half in range(column_pole.shape[0]):
        send, keep, coeff = panel_half(side, pole, weight, panel, eigen, half, rows, prepared, tiles)
        coeffs.append(coeff)
        met = lax.ppermute(send, "row", near_pairs)
        own, *blocks = merge(deep, keep, met)
        arrived = [own]
        for shift, block in enumerate(blocks, 1):
            pairs = [(r, (r + 2 * shift) % rows) for r in range(rows)]
            arrived.append(lax.ppermute(block, "row", pairs))
        outgoing.append(blocks)
        received.append(arrived)

    members = coeffs[0].shape[0]
    groups = [coeffs] if members == tiles else [[c] for c in coeffs]
    calls = [(g, step) for g in range(len(groups)) for step in range(ITERS)]
    lates = {1: outgoing[0], len(calls) // 2: outgoing[1]}
    latest = []
    spread = my_offsets.reshape(tiles, 1, LANES)
    nows = [spread[g * members : (g + 1) * members] for g in range(len(groups))]
    for at, (g, step) in enumerate(calls):
        nows[g] = update(prepared, all_poles, all_weights, my_centers, nows[g], my_first, g * members, groups[g], latest + lates.get(at, []))
        latest = [nows[g]]
    my_offsets = jnp.concatenate(nows, axis=0)
    offset_now = gather([(flat(my_offsets), ("row",))], 2)[0].reshape(-1)
    add = lambda parts: sum([p.astype(jnp.float32) for p in parts[1:]], parts[0])
    halves = [add(parts) for parts in received]
    return (offset_now, jnp.stack(halves, axis=1))


def copies(value, axis, count):
    return lax.all_to_all(jnp.broadcast_to(value[None], (count,) + value.shape), axis, 0, 0, tiled=True)


def gather_inputs(pole_values, weights, offsets, rows, cols):
    both = copies(jnp.stack([pole_values.reshape(-1, LANES), weights.reshape(-1, LANES)]), "row", rows)
    own = offsets.reshape(-1, LANES)
    turned = [own] + [lax.ppermute(own, "col", [(c, (c + shift) % cols) for c in range(cols)]) for shift in range(1, cols)]
    return both[:, 0].reshape(-1), both[:, 1].reshape(-1), jnp.concatenate(turned, axis=0)


def solution(mesh):
    placed = (P("row"), P("row"), P("col"), P("col"), P(), P(None, "row"), P("col", None, "row"))

    return jax.shard_map(
        on_device,
        mesh=mesh,
        in_specs=placed,
        out_specs=(P("col"), P(("col", "row"), None, None)),
        check_vma=False,
    )
```

```python
import functools
import itertools
import jax
import jax.numpy as jnp
from jax import lax
from jax.experimental import pallas as pl
from jax.experimental.pallas import tpu as pltpu
from jax.sharding import PartitionSpec as P

AXES = ("row", "col")
LANES = 128
ITERS = 3
BLOCK = 32
TERMS = 40
KAPPA = 4.0
PAIR = 2
PIECES = 3
WIDTH = 256
DEPTH = 1024
FLOPS_PER_US = 1_000_000_000


def power(base, exponent):
    result = jnp.ones_like(base)
    square = base
    for bit in range(6):
        result = jnp.where((exponent >> bit) & 1 == 1, result * square, result)
        square = square * square
    return result


def pieces(values):
    high = values.astype(jnp.bfloat16).astype(jnp.float32)
    return high, values - high


def gather(items, collective_id):
    sizes = {axis: lax.axis_size(axis) for axis in AXES}
    offsets_of = lambda axes: list(itertools.product(*[range(sizes[a]) if a in axes else (0,) for a in AXES]))
    groups = [offsets_of(axes) for _, axes in items]
    greeted = sorted({offset for group in groups for offset in group[1:]})
    count = len(items)

    def kernel(*refs):
        sources, targets, send, receive = refs[:count], refs[count : 2 * count], refs[2 * count], refs[2 * count + 1]
        here = [lax.axis_index(axis) for axis in AXES]
        device = lambda offset: tuple(lax.rem(h + o, sizes[a]) for h, o, a in zip(here, offset, AXES))
        barrier = pltpu.get_barrier_semaphore()
        for offset in greeted:
            pl.semaphore_signal(barrier, inc=1, device_id=device(offset), device_id_type=pl.DeviceIdType.MESH)
        pl.semaphore_wait(barrier, len(greeted))
        copies = []
        for (_, axes), group, source, target in zip(items, groups, sources, targets):
            slot = 0
            for h, a in zip(here, AXES):
                if a in axes:
                    slot = slot * sizes[a] + h
            for offset in group[1:]:
                copies.append(
                    pltpu.make_async_remote_copy(
                        src_ref=source,
                        dst_ref=target.at[slot],
                        send_sem=send.at[len(copies)],
                        recv_sem=receive.at[len(copies)],
                        device_id=device(offset),
                        device_id_type=pl.DeviceIdType.MESH,
                    )
                )
                copies[-1].start()
            target[slot] = source[...]
        for copy in copies:
            copy.wait()

    total = sum(len(group) - 1 for group in groups)
    vmem = pl.BlockSpec(memory_space=pltpu.VMEM)
    return pl.pallas_call(
        kernel,
        out_shape=[jax.ShapeDtypeStruct((len(g),) + v.shape, v.dtype) for (v, _), g in zip(items, groups)],
        in_specs=[vmem] * count,
        out_specs=[vmem] * count,
        scratch_shapes=[pltpu.SemaphoreType.DMA((total,)), pltpu.SemaphoreType.DMA((total,))],
        compiler_params=pltpu.CompilerParams(collective_id=collective_id, has_side_effects=True),
        name="gather",
    )(*[v for v, _ in items])


def coefficients(geometry, poles, weights, q, coeff_ref, at, top_ref, bottom_ref):
    blank = jnp.zeros((8, LANES), jnp.float32)
    for k in range(BLOCK, TERMS):
        top_ref[8 * k : 8 * k + 8, :] = blank
        bottom_ref[8 * k : 8 * k + 8, :] = blank
    middle, radius, first, last = geometry
    inverse_radius = 1.0 / radius
    top, bottom = [], [jnp.ones((8, LANES), jnp.float32)]
    for j in range(BLOCK):
        weight = weights[j : j + 1, :]
        row = (q * BLOCK + j).astype(jnp.float32)
        scale = jnp.where(jnp.logical_or(row < first, row >= last), radius, 0.0)
        ratio = scale / (poles[j : j + 1, :] - middle)
        value = (weight * weight) * ratio * inverse_radius
        new_top, new_bottom = [], []
        for k in range(j + 1):
            term = value * bottom[k]
            if k < j:
                term = top[k] + term
            if k > 0:
                term = term - ratio * top[k - 1]
            new_top.append(term)
        for k in range(j + 2):
            term = bottom[k] if k <= j else None
            if k > 0:
                shifted = ratio * bottom[k - 1]
                term = -shifted if term is None else term - shifted
            new_bottom.append(term)
        top, bottom = new_top, new_bottom
    for k in range(BLOCK):
        top_ref[8 * k : 8 * k + 8, :] = top[k]
    for k in range(BLOCK + 1):
        bottom_ref[8 * k : 8 * k + 8, :] = bottom[k]
    for member in range(coeff_ref.shape[0]):
        for ref, lane in ((top_ref, 0), (bottom_ref, LANES)):
            high, low = pieces(ref[pl.ds(member, TERMS, stride=8), :])
            rows = jnp.concatenate([high, low, high, blank], axis=0)
            coeff_ref[member, at, :, lane : lane + LANES] = rows.astype(jnp.bfloat16)


def update_kernel(count, base, near_ref, middle_ref, radius_ref, first_ref, poles_ref, weights_ref, center_ref, offset_ref, *refs):
    coeff_refs, out_ref = refs[:count], refs[-1]
    tile = base + pl.program_id(0)
    order = lax.broadcasted_iota(jnp.int32, (TERMS, LANES), 0)
    blank = jnp.zeros((8, LANES), jnp.float32)

    def to_rows(values):
        high, low = pieces(values)
        return jnp.concatenate([high, high, low, blank], axis=0).T.astype(jnp.bfloat16)

    center = center_ref[0]
    middle, radius = middle_ref[tile], radius_ref[tile]

    def step(_, offset):
        place = (center - middle) + offset
        ratio = jnp.broadcast_to(place / radius, (TERMS, LANES))
        value_rows = to_rows(power(ratio, order))
        slope_rows = to_rows(order.astype(jnp.float32) * power(ratio, jnp.maximum(order - 1, 0)))
        rows = jnp.concatenate([value_rows, slope_rows], axis=0)
        inverse_sum = square_sum = None
        for ref, q in [(ref, q) for ref in coeff_refs for q in range(ref.shape[1])]:
            got = jnp.dot(rows, ref[0, q], preferred_element_type=jnp.float32)
            top, bottom = got[:LANES, :LANES], got[:LANES, LANES:]
            top_slope, bottom_slope = got[LANES:, :LANES], got[LANES:, LANES:]
            inverse = 1.0 / bottom
            quotient = top * inverse
            slope = (top_slope - quotient * bottom_slope) * inverse
            inverse_sum = quotient if inverse_sum is None else inverse_sum + quotient
            square_sum = slope if square_sum is None else square_sum + slope
        square_sum = square_sum / radius
        place_rows = jnp.broadcast_to(place, (LANES, LANES)).T
        inverse_parts, square_parts = [], []
        half = LANES // 2
        for part in range(2):
            own = slice(part * half, (part + 1) * half)
            points = place_rows[own]

            def near(step, sums):
                inverse_sum, square_sum = sums
                for i in range(PAIR):
                    row = step * PAIR + i
                    pole = poles_ref[pl.ds(row, 1), :] - middle
                    weight = weights_ref[pl.ds(row, 1), :]
                    inverse = 1.0 / (pole - points)
                    weighted = (weight * weight) * inverse
                    inverse_sum = inverse_sum + weighted
                    square_sum = square_sum + weighted * inverse
                return inverse_sum, square_sum

            sums = lax.fori_loop(near_ref[0, tile], near_ref[1, tile], near, (inverse_sum[own], square_sum[own]))
            inverse_parts.append(sums[0])
            square_parts.append(sums[1])
        total = lambda parts: jnp.sum(jnp.concatenate(parts, axis=0).T, axis=0, keepdims=True)
        sum_inverse, sum_square = total(inverse_parts), total(square_parts)
        row = first_ref[0] + tile
        to_left = poles_ref[pl.ds(row, 1), :] - center
        final = lax.broadcasted_iota(jnp.int32, (1, LANES), 1) + row * LANES == poles_ref.shape[0] * LANES - 1
        to_right = jnp.where(final, to_left, -to_left)
        limit = 0.5 * jnp.minimum(jnp.abs(to_left - offset), jnp.abs(to_right - offset))
        change = (1.0 + sum_inverse) / sum_square
        return offset - jnp.minimum(jnp.maximum(change, -limit), limit)

    out_ref[0] = lax.fori_loop(0, ITERS, step, offset_ref[0])


def prepare(poles, weights, centers):
    flat = lambda values: values.reshape(-1, LANES)
    tiles = centers.shape[0] // LANES
    tile_centers = flat(centers)
    middle = tile_centers[:, LANES // 2]
    radius = jnp.maximum(tile_centers[:, -1] - middle, middle - tile_centers[:, 0]) + 2.5
    below = jnp.sum((poles[None, :] <= (middle - KAPPA * radius)[:, None]).astype(jnp.int32), axis=1)
    inside = jnp.sum((poles[None, :] < (middle + KAPPA * radius)[:, None]).astype(jnp.int32), axis=1)
    unit = PAIR * LANES
    near = jnp.stack([below // unit, (inside + unit - 1) // unit])
    limits = (near * PAIR).astype(jnp.float32)
    geometry = jnp.stack([middle, radius, limits[0], limits[1]])
    geometry = jnp.pad(geometry, ((0, 0), (0, -tiles % 8)), mode="edge")
    geometry = jnp.broadcast_to(geometry[:, :, None], geometry.shape + (LANES,))
    return near, middle, radius, geometry, flat(poles), flat(weights)


def update(prepared, centers, offsets, my_first, base, first, size, coeffs, after):
    near, middle, radius, _, poles, weights = prepared
    smem, anywhere = pl.BlockSpec(memory_space=pltpu.SMEM), pl.BlockSpec(memory_space=pl.ANY)
    whole = pl.BlockSpec(poles.shape, lambda t: (0, 0))
    one = pl.BlockSpec((1, 1, LANES), lambda t: (base + t, 0, 0))
    spread = lambda values: values.reshape(-1, 1, LANES)
    return pl.pallas_call(
        functools.partial(update_kernel, len(coeffs), base),
        grid=(size,),
        out_shape=jax.ShapeDtypeStruct((size, 1, LANES), jnp.float32),
        in_specs=[smem] * 4
        + [whole] * 2
        + [one] * 2
        + [pl.BlockSpec((1,) + c.shape[1:], lambda t: (first + t, 0, 0, 0)) for c in coeffs]
        + [anywhere] * len(after),
        out_specs=pl.BlockSpec((1, 1, LANES), lambda t: (t, 0, 0)),
        cost_estimate=pl.CostEstimate(flops=FLOPS_PER_US * 15, bytes_accessed=size * LANES * LANES * 64, transcendentals=0),
        name="update",
    )(near, middle, radius, (my_first // LANES).reshape(1), poles, weights, spread(centers), spread(offsets), *coeffs, *after)


def lookup_kernel(index_ref, *refs):
    count = (len(refs) - 1) // 2
    tables, targets, pieces_ref = refs[:count], refs[count : 2 * count], refs[2 * count]
    rows = tables[0].shape[0]

    @pl.when(pl.program_id(0) == 0)
    def _():
        for t, table in enumerate(tables):
            rest = table[...]
            for p in range(PIECES):
                part = rest.astype(jnp.bfloat16)
                at = (t * PIECES + p) * LANES
                pieces_ref[:, at : at + LANES] = part
                rest = rest - part.astype(jnp.float32)

    lane = lax.broadcasted_iota(jnp.int32, (LANES, LANES), 1)
    for g in range(index_ref.shape[0]):
        index = jnp.broadcast_to(index_ref[g], (LANES, LANES)).T
        high = lax.shift_right_logical(index, 7)
        low = lax.bitwise_and(index, LANES - 1)
        pick = jnp.concatenate([(high == lane + c * LANES).astype(jnp.float32) for c in range(rows // LANES)], axis=1)
        found = jnp.dot(pick.astype(jnp.bfloat16), pieces_ref[...], preferred_element_type=jnp.float32)
        for t, target in enumerate(targets):
            parts = [found[:, (t * PIECES + p) * LANES : (t * PIECES + p + 1) * LANES] for p in range(PIECES)]
            value = (parts[0] + parts[1]) + parts[2]
            value = jnp.sum(jnp.where(low == lane, value, 0.0), axis=1, keepdims=True)
            target[g * LANES : (g + 1) * LANES, :] = jnp.broadcast_to(value, (LANES, LANES))


def lookup(tables, index):
    groups = index.shape[0] // LANES
    step = min(groups, 8)
    count = len(tables)
    return pl.pallas_call(
        lookup_kernel,
        grid=(groups // step,),
        out_shape=[jax.ShapeDtypeStruct((index.shape[0], LANES), jnp.float32)] * count,
        in_specs=[pl.BlockSpec((step, 1, LANES), lambda i: (i, 0, 0))] + [pl.BlockSpec(t.shape, lambda i: (0, 0)) for t in tables],
        out_specs=[pl.BlockSpec((step * LANES, LANES), lambda i: (i, 0))] * count,
        scratch_shapes=[pltpu.VMEM((tables[0].shape[0], count * PIECES * LANES), jnp.bfloat16)],
        name="lookup",
    )(index.reshape(groups, 1, LANES), *tables)


def chosen_kernel(count, poles_ref, weights_ref, found_ref, start_ref, out_ref):
    left, right = found_ref[:count], found_ref[LANES : LANES + count]
    center = jnp.where(left == right, left + 0.5, 0.5 * (left + right))
    to_left, to_right = left - center, right - center
    rows = poles_ref.shape[0]

    def sweep(offset, square_only):
        def row(index, sums):
            inverse = 1.0 / ((poles_ref[pl.ds(index, 1), :] - center) - offset)
            weight = weights_ref[pl.ds(index, 1), :]
            weighted = (weight * weight) * inverse
            square_sum = sums[1] + weighted * inverse
            return (sums[0] if square_only else sums[0] + weighted), square_sum

        zero = jnp.zeros_like(center)
        sums = lax.fori_loop(0, rows, row, (zero, zero), unroll=8)
        return [jnp.broadcast_to(jnp.sum(s, axis=1, keepdims=True), center.shape) for s in sums]

    def step(_, offset):
        sum_inverse, sum_square = sweep(offset, False)
        limit = 0.5 * jnp.minimum(jnp.abs(to_left - offset), jnp.abs(to_right - offset))
        change = (1.0 + sum_inverse) / sum_square
        return offset - jnp.minimum(jnp.maximum(change, -limit), limit)

    offset = lax.fori_loop(0, ITERS, step, start_ref[2 * LANES : 2 * LANES + count])
    norm = lax.rsqrt(sweep(offset, True)[1])
    lane = lax.broadcasted_iota(jnp.int32, (count, LANES), 1)
    own = lane == lax.broadcasted_iota(jnp.int32, (count, LANES), 0)
    spread = lambda values: jnp.sum(jnp.where(own, values, 0.0), axis=0, keepdims=True)
    blank = jnp.zeros((5, LANES), jnp.float32)
    out_ref[...] = jnp.concatenate([spread(center), spread(offset), spread(norm), blank], axis=0)


def panel_kernel(start, chunks, side_ref, pole_ref, weight_ref, center_ref, offset_ref, norm_ref, eigen_ref, geometry_ref, block_poles_ref, block_weights_ref, send_ref, keep_ref, coeff_ref, total_ref, *refs):
    depth = eigen_ref.shape[2]
    center, offset, norm = center_ref[...], offset_ref[...], norm_ref[...]
    total = None
    for first in range(0, depth, DEPTH):
        rows = slice(first, first + DEPTH)
        columns = []
        for at in range(0, WIDTH, LANES):
            lanes = slice(at, at + LANES)
            distance = (pole_ref[rows, :] - center[:, lanes]) - offset[:, lanes]
            columns.append((weight_ref[rows, :] * (1.0 / distance) * norm[:, lanes]).astype(jnp.bfloat16))
        part = jnp.dot(eigen_ref[0, :, rows], jnp.concatenate(columns, axis=1), preferred_element_type=jnp.float32)
        total = part if total is None else total + part
    per = coeff_ref.shape[1]
    for u in range(per):
        q = lax.rem(start + pl.program_id(0) * per + u, chunks)
        geometry = [geometry_ref[i] for i in range(4)]
        own = pl.ds(u * BLOCK, BLOCK)
        coefficients(geometry, block_poles_ref[own, :], block_weights_ref[own, :], q, coeff_ref, u, *refs[2 * u : 2 * u + 2])
    total_ref[...] = total
    side = side_ref[0]
    size = send_ref.shape[1]
    for z in range(send_ref.shape[0]):
        send_ref[z] = total_ref[pl.ds(pl.multiple_of((2 * z + 1 - side) * size, 8), size), :].astype(jnp.bfloat16)
        keep_ref[z] = total_ref[pl.ds(pl.multiple_of((2 * z + side) * size, 8), size), :]


def panel_half(side, pole, weight, panel, eigen, half, rows, prepared, tiles):
    height, depth = eigen.shape[1], eigen.shape[2]
    width = panel[0].shape[0]
    steps = width // WIDTH
    geometry, block_poles, block_weights = prepared[3:]
    chunks = block_poles.shape[0] // BLOCK
    octets = geometry.shape[1] // 8
    per = octets * chunks // (eigen.shape[0] * steps)
    start = half * steps * per
    octet, members = start // chunks, min(tiles, 8)
    shape = (rows // 2, height // rows, width)
    row = pl.BlockSpec((1, WIDTH), lambda i: (0, i))
    wide = pl.BlockSpec((depth, LANES), lambda i: (half, 0))
    out = pl.BlockSpec(shape[:2] + (WIDTH,), lambda i: (0, 0, i))
    blocks = pl.BlockSpec((per * BLOCK, LANES), lambda i: (start % chunks // per + i, 0))
    return pl.pallas_call(
        functools.partial(panel_kernel, start, chunks),
        grid=(steps,),
        out_shape=[
            jax.ShapeDtypeStruct(shape, jnp.bfloat16),
            jax.ShapeDtypeStruct(shape, jnp.float32),
            jax.ShapeDtypeStruct((members, steps * per, LANES, 2 * LANES), jnp.bfloat16),
        ],
        in_specs=[pl.BlockSpec(memory_space=pltpu.SMEM), wide, wide, row, row, row, pl.BlockSpec((1, height, depth), lambda i: (half, 0, 0))]
        + [pl.BlockSpec((4, 8, LANES), lambda i: (0, octet, 0)), blocks, blocks],
        out_specs=[out, out, pl.BlockSpec((members, per, LANES, 2 * LANES), lambda i: (0, i, 0, 0))],
        scratch_shapes=[pltpu.VMEM((height, WIDTH), jnp.float32)] + [pltpu.VMEM((8 * TERMS, LANES), jnp.float32)] * (2 * per),
        cost_estimate=pl.CostEstimate(flops=FLOPS_PER_US * 22, bytes_accessed=height * depth * 2, transcendentals=0),
        compiler_params=pltpu.CompilerParams(vmem_limit_bytes=60 * 1024 * 1024),
        name="panel",
    )(side, pole, weight, *[p[None, :] for p in panel], eigen, geometry, block_poles, block_weights)


def merge_kernel(deep_ref, keep_ref, met_ref, own_ref, *block_refs):
    count = keep_ref.shape[0]
    deep = deep_ref[0]
    for shift, ref in enumerate((own_ref,) + block_refs):
        at = lax.rem(deep + shift, count)
        ref[...] = (keep_ref[at] + met_ref[at].astype(jnp.float32)).astype(ref.dtype)


def merge(deep, keep, met):
    count, height, width = keep.shape
    size = WIDTH * 2
    whole = pl.BlockSpec((count, height, size), lambda i: (0, 0, i))
    block = pl.BlockSpec((height, size), lambda i: (0, i))
    return pl.pallas_call(
        merge_kernel,
        grid=(width // size,),
        out_shape=[jax.ShapeDtypeStruct((height, width), jnp.bfloat16 if s else jnp.float32) for s in range(count)],
        in_specs=[pl.BlockSpec(memory_space=pltpu.SMEM), whole, whole],
        out_specs=[block] * count,
        cost_estimate=pl.CostEstimate(flops=FLOPS_PER_US * 2, bytes_accessed=keep.size * 8, transcendentals=0),
        name="merge",
    )(deep.reshape(1), keep, met)


def on_device(pole_values, weights, centers, offsets, chosen, column_pole, eigen_blocks):
    flat = lambda values: values.reshape(-1, LANES)
    rows, cols = lax.axis_size("row"), lax.axis_size("col")
    row, col = lax.axis_index("row"), lax.axis_index("col")
    per_device = offsets.shape[0] // rows
    first_root = row * per_device
    my_first = col * offsets.shape[0] + first_root
    all_poles, all_weights, all_offsets = gather_inputs(pole_values, weights, offsets, rows, cols)
    total = all_poles.shape[0]

    share = chosen.shape[0] // (rows * cols)
    mine = lax.dynamic_slice_in_dim(chosen, (row * cols + col) * share, share)
    padded = jnp.pad(mine, (0, LANES - share))
    per_col = offsets.shape[0]
    turned = lax.rem(col - padded // per_col + cols, cols) * per_col + lax.rem(padded, per_col)
    index = jnp.concatenate([padded, jnp.minimum(padded + 1, total - 1), turned])
    found_pole, found_offset = lookup([flat(all_poles), all_offsets], index)
    here = pl.BlockSpec(memory_space=pltpu.VMEM)
    packed = pl.pallas_call(
        functools.partial(chosen_kernel, share), out_shape=jax.ShapeDtypeStruct((8, LANES), jnp.float32), in_specs=[here] * 4, out_specs=here, name="chosen"
    )(flat(all_poles), flat(all_weights), found_pole, found_offset)
    shared = copies(packed, AXES, rows * cols)
    panel = shared[:, :3, :share].transpose(1, 0, 2).reshape(3, -1)

    pole, weight = lookup([flat(all_poles), flat(all_weights)], column_pole.reshape(-1))
    eigen = jnp.transpose(eigen_blocks, (1, 0, 2))
    side = lax.rem(row, 2).reshape(1)
    deep = row // 2
    near_pairs = [(r, r ^ 1) for r in range(rows)]
    my_centers = lax.dynamic_slice_in_dim(centers, first_root, per_device)
    my_offsets = lax.dynamic_slice_in_dim(offsets, first_root, per_device)
    prepared = prepare(all_poles, all_weights, my_centers)
    tiles = per_device // LANES
    received, outgoing, coeffs = [], [], []
    for half in range(column_pole.shape[0]):
        send, keep, coeff = panel_half(side, pole, weight, panel, eigen, half, rows, prepared, tiles)
        coeffs.append(coeff)
        met = lax.ppermute(send, "row", near_pairs)
        own, *blocks = merge(deep, keep, met)
        arrived = [own]
        for shift, block in enumerate(blocks, 1):
            pairs = [(r, (r + 2 * shift) % rows) for r in range(rows)]
            arrived.append(lax.ppermute(block, "row", pairs))
        outgoing.append(blocks)
        received.append(arrived)

    members = coeffs[0].shape[0]
    groups = [coeffs] if members == tiles else [[c] for c in coeffs]
    size = max(members // 2, 1)
    calls = [(g, first) for g in range(len(groups)) for first in range(0, members, size)]
    lates = {1: outgoing[0], 2: outgoing[1]}
    found, latest = [], []
    for at, (g, first) in enumerate(calls):
        after = latest + lates.get(at, [])
        latest = [update(prepared, my_centers, my_offsets, my_first, g * members + first, first, size, groups[g], after)]
        found += latest
    my_offsets = jnp.concatenate(found, axis=0)
    offset_now = gather([(flat(my_offsets), ("row",))], 2)[0].reshape(-1)
    add = lambda parts: sum([p.astype(jnp.float32) for p in parts[1:]], parts[0])
    halves = [add(parts) for parts in received]
    return (offset_now, jnp.stack(halves, axis=1))


def copies(value, axis, count):
    return lax.all_to_all(jnp.broadcast_to(value[None], (count,) + value.shape), axis, 0, 0, tiled=True)


def gather_inputs(pole_values, weights, offsets, rows, cols):
    both = copies(jnp.stack([pole_values.reshape(-1, LANES), weights.reshape(-1, LANES)]), "row", rows)
    own = offsets.reshape(-1, LANES)
    turned = [own] + [lax.ppermute(own, "col", [(c, (c + shift) % cols) for c in range(cols)]) for shift in range(1, cols)]
    return both[:, 0].reshape(-1), both[:, 1].reshape(-1), jnp.concatenate(turned, axis=0)


def solution(mesh):
    placed = (P("row"), P("row"), P("col"), P("col"), P(), P(None, "row"), P("col", None, "row"))

    return jax.shard_map(
        on_device,
        mesh=mesh,
        in_specs=placed,
        out_specs=(P("col"), P(("col", "row"), None, None)),
        check_vma=False,
    )
```
